32 devices in a mesh: dp: 32 (over z, y, x, core).
Axes of the slice: x: 2, y: 2, z: 4, core: 2. Of those that a mesh axis runs over, the one named last changes fastest.
Arguments:
- grad_proj: bfloat16 [32, 3, 512, 512], P('dp')
- grad_up: bfloat16 [32, 3, 512, 2048], P('dp')
- err_proj: float32 [32, 3, 512, 512], P('dp')
- err_up: float32 [32, 3, 512, 2048], P('dp')
- q_proj: float32 [3, 512, 64], replicated
- q_up: float32 [3, 2048, 64], replicated
- w_proj: float32 [3, 512, 512], replicated
- w_up: float32 [3, 512, 2048], replicated
- mom_proj: float32 [3, 512, 512], replicated
- mom_up: float32 [3, 512, 2048], replicated
Outputs:
- output 1: float32 [3, 512, 512], replicated
- output 2: float32 [3, 512, 2048], replicated
- output 3: float32 [3, 512, 512], replicated
- output 4: float32 [3, 512, 2048], replicated
- output 5: float32 [3, 512, 64], replicated
- output 6: float32 [3, 2048, 64], replicated
- output 7: float32 [32, 3, 512, 512], P('dp')
- output 8: float32 [32, 3, 512, 2048], P('dp')
All inputs are finite; a program needn't handle non-finite values.
Results may differ from the reference program's by a relative error of at most 0.001.
Values sent between devices are 32-bit elements.
A program may use at most 1 GiB of HBM per device.

```python
import jax
import jax.numpy as jnp
from jax import lax

NUM_DEV = 32
LAYERS = 3
D = 512
FF = 2048
RANK = 64
MOMENTUM = 0.9
LEARN_RATE = 0.1
PRECISE = lax.Precision.HIGHEST


def orthonormalize(p_mat):
    col_ids = jnp.arange(p_mat.shape[1])

    def gs_step(index, p_cur):
        col_vec = lax.dynamic_slice_in_dim(p_cur, index, 1, axis=1)
        unit_vec = col_vec / jnp.sqrt(jnp.sum(col_vec * col_vec))
        coeffs = jnp.sum(unit_vec * p_cur, axis=0, keepdims=True)
        later = (col_ids > index)[None, :]
        p_cur = p_cur - unit_vec * jnp.where(later, coeffs, 0.0)
        return jnp.where((col_ids == index)[None, :], unit_vec, p_cur)

    return lax.fori_loop(0, p_mat.shape[1], gs_step, p_mat)


def layer_step(operands):
    grad_l, err_l, q_l, w_l, mom_l = operands
    m_all = grad_l.astype(jnp.float32) + err_l
    p_all = jnp.einsum('dmn,nr->dmr', m_all, q_l, precision=PRECISE)
    p_mat = orthonormalize(jnp.mean(p_all, axis=0))
    q_all = jnp.einsum('dmn,mr->dnr', m_all, p_mat, precision=PRECISE)
    q_new = jnp.mean(q_all, axis=0)
    g_hat = jnp.dot(p_mat, q_new.T, precision=PRECISE)
    err_new = m_all - g_hat[None]
    mom_new = MOMENTUM * mom_l + g_hat
    w_new = w_l - LEARN_RATE * mom_new
    return w_new, mom_new, q_new, err_new


def compress_all(grad_all, err_all, q_factor, weights, moment_in):
    w_new, mom_new, q_new, err_new = lax.map(layer_step, (jnp.swapaxes(grad_all, 0, 1), jnp.swapaxes(err_all, 0, 1), q_factor, weights, moment_in))
    return w_new, mom_new, q_new, jnp.swapaxes(err_new, 0, 1)


def draw_grad(key, rows, cols):
    spec_len = 4 * RANK + 16
    key_list = jax.random.split(key, 5)
    decay = (1.0 + jnp.arange(spec_len).astype(jnp.float32) / RANK) ** (-1.5)
    decay = decay / jnp.sqrt(jnp.sum(decay * decay))
    left_sh = jax.random.normal(key_list[0], (LAYERS, rows, spec_len), jnp.float32) * decay
    right_sh = jax.random.normal(key_list[1], (LAYERS, cols, spec_len), jnp.float32)
    shared = jnp.einsum('lmk,lnk->lmn', left_sh, right_sh)
    left_dev = jax.random.normal(key_list[2], (NUM_DEV, LAYERS, rows, spec_len), jnp.float32) * decay
    right_dev = jax.random.normal(key_list[3], (NUM_DEV, LAYERS, cols, spec_len), jnp.float32)
    own_part = jnp.einsum('dlmk,dlnk->dlmn', left_dev, right_dev)
    noise = jax.random.normal(key_list[4], (NUM_DEV, LAYERS, rows, cols), jnp.float32)
    return (shared[None] + 0.7 * own_part + 0.3 * noise).astype(jnp.bfloat16)


def setup_inputs(seed: int = 0) -> dict:
    key_list = jax.random.split(jax.random.key(seed), 10)
    return {
        'grad_proj': draw_grad(key_list[0], D, D),
        'grad_up': draw_grad(key_list[1], D, FF),
        'err_proj': 0.5 * jax.random.normal(key_list[2], (NUM_DEV, LAYERS, D, D), jnp.float32),
        'err_up': 0.5 * jax.random.normal(key_list[3], (NUM_DEV, LAYERS, D, FF), jnp.float32),
        'q_proj': jax.random.normal(key_list[4], (LAYERS, D, RANK), jnp.float32),
        'q_up': jax.random.normal(key_list[5], (LAYERS, FF, RANK), jnp.float32),
        'w_proj': jax.random.normal(key_list[6], (LAYERS, D, D), jnp.float32) * D ** -0.5,
        'w_up': jax.random.normal(key_list[7], (LAYERS, D, FF), jnp.float32) * D ** -0.5,
        'mom_proj': 0.5 * jax.random.normal(key_list[8], (LAYERS, D, D), jnp.float32),
        'mom_up': 0.5 * jax.random.normal(key_list[9], (LAYERS, D, FF), jnp.float32),
    }


def reference(grad_proj, grad_up, err_proj, err_up, q_proj, q_up, w_proj, w_up, mom_proj, mom_up):
    proj = compress_all(grad_proj, err_proj, q_proj, w_proj, mom_proj)
    upper = compress_all(grad_up, err_up, q_up, w_up, mom_up)
    return (proj[0], upper[0], proj[1], upper[1], proj[2], upper[2], proj[3], upper[3])
```

```python
import jax
import jax.numpy as jnp
from jax import lax
from jax.experimental import pallas as pl
from jax.experimental.pallas import tpu as pltpu
from jax.sharding import PartitionSpec as P

MOMENTUM = 0.9
LEARN_RATE = 0.1
F32 = jnp.float32
BF16 = jnp.bfloat16
MESH = pl.DeviceIdType.MESH
LAYERS = 3
RANK = 64
BLK = 512
HALF = 256
PER_LAYER = 5
CHUNKS = LAYERS * PER_LAYER
SLOTS = 4
VMEM_LIMIT = 14 << 20
P_COLS = 1024
Q_COLS = 2560
NT = (((1,), (1,)), ((), ()))
NN = (((1,), (0,)), ((), ()))


def split3(val):
    one = val.astype(BF16)
    rest = val - one.astype(F32)
    two = rest.astype(BF16)
    three = (rest - two.astype(F32)).astype(BF16)
    return one, two, three


def mxu(lhs, rhs, dims):
    return lax.dot_general(lhs, rhs, dims, preferred_element_type=F32)


def stacked_dot(fac, mat, dims):
    f1, f2, f3 = split3(fac)
    m1, m2, m3 = split3(mat)
    stack = jnp.concatenate([f1, f2, f3], axis=0)
    d1 = mxu(stack, m1, dims)
    d2 = mxu(stack[: 2 * RANK], m2, dims)
    d3 = mxu(stack[:RANK], m3, dims)
    low = d1[2 * RANK :] + d2[RANK:] + d3
    mid = d1[RANK : 2 * RANK] + d2[:RANK]
    return d1[:RANK] + (mid + low)


def full_dot(lhs, rhs, dims):
    return lax.dot_general(lhs, rhs, dims, precision=lax.Precision.HIGHEST, preferred_element_type=F32)


class Unit:
    def __init__(self, place, parts, result, sems, num_dev):
        self.x, self.ra, self.rb, self.rc, self.r = parts + (result,)
        self.ssem, self.rsem = sems
        self.num_dev = num_dev
        self.cols = self.x.shape[1]
        self.zc = self.cols // 4
        self.place = place
        self.sends = []

    def copy(self, src, dst, idx, dev):
        return pltpu.make_async_remote_copy(
            src_ref=src, dst_ref=dst, send_sem=self.ssem.at[idx], recv_sem=self.rsem.at[idx],
            device_id=(dev,), device_id_type=MESH)

    def start(self, cps):
        for cp in cps:
            cp.start()
        self.sends += cps

    def zcols(self, z):
        return pl.ds(pl.multiple_of(z * self.zc, 128), self.zc)

    def stage(self, num):
        p = self.place
        if num == 0:
            self.a = self.copy(self.x.at[pl.ds(p.other_half, 32)], self.ra, 0, p.partner)
            self.start([self.a])
        elif num == 1:
            self.a.wait_recv()
            self.ra[...] += self.x[pl.ds(p.half, 32)]
            self.b = [self.copy(self.ra.at[pl.ds(p.mate_sub[k], 8)], self.rb.at[k], 1 + k, p.mates[k]) for k in range(3)]
            self.start(self.b)
        elif num == 2:
            own = self.ra[pl.ds(p.sub, 8)]
            for cp in self.b:
                cp.wait_recv()
            self.x[pl.ds(p.row, 8)] = (own + self.rb[0]) + (self.rb[1] + self.rb[2])
            self.c = [self.copy(self.x.at[pl.ds(p.row, 8), self.zcols(p.zs[k])], self.rc.at[k], 4 + k, p.zmates[k]) for k in range(3)]
            self.start(self.c)
        elif num == 3:
            own = self.x[pl.ds(p.row, 8), self.zcols(p.z)]
            for cp in self.c:
                cp.wait_recv()
            tot = (own + self.rc[0]) + (self.rc[1] + self.rc[2])
            self.r[pl.ds(p.row, 8), self.zcols(p.z)] = tot * (1.0 / self.num_dev)
            ref = self.r.at[pl.ds(p.row, 8), self.zcols(p.z)]
            self.d = [self.copy(ref, ref, 7 + k, p.zmates[k]) for k in range(3)]
            self.start(self.d)
        elif num == 4:
            for cp in self.d:
                cp.wait_recv()
            ref = self.r.at[pl.ds(p.row, 8)]
            self.e = [self.copy(ref, ref, 10 + k, p.mates[k]) for k in range(3)]
            self.start(self.e)
        elif num == 5:
            for cp in self.e:
                cp.wait_recv()
            ref = self.r.at[pl.ds(p.half, 32)]
            self.f = self.copy(ref, ref, 13, p.partner)
            self.start([self.f])
        else:
            self.f.wait_recv()

    def finish(self):
        for cp in self.sends:
            cp.wait_send()


class Place:
    def __init__(self):
        me = lax.axis_index('dp')
        core, x, y, z = me % 2, (me // 2) % 2, (me // 4) % 2, me // 8
        dx, dy = 2 - 4 * x, 4 - 8 * y
        self.z = z
        self.partner = me + 1 - 2 * core
        self.mates = [me + dx, me + dy, me + dx + dy]
        self.zs = [(z + k) % 4 for k in (1, 2, 3)]
        self.zmates = [me + 8 * (zk - z) for zk in self.zs]
        self.half = pl.multiple_of(core * 32, 32)
        self.other_half = pl.multiple_of(32 - core * 32, 32)
        sub = x + 2 * y
        self.sub = pl.multiple_of(sub * 8, 8)
        self.mate_sub = [pl.multiple_of(((1 - x) + 2 * y) * 8, 8), pl.multiple_of((x + 2 * (1 - y)) * 8, 8),
                         pl.multiple_of(((1 - x) + 2 * (1 - y)) * 8, 8)]
        self.row = pl.multiple_of(core * 32 + sub * 8, 8)


def eliminate(aug):
    rows = RANK
    for base in range(0, rows, 8):
        r = [aug[base + i] for i in range(8)]
        d = {}
        for i in range(8):
            for j in range(i, 8):
                d[i, j] = jnp.broadcast_to(r[i][:, base + j : base + j + 1], (8, 128))
        inv = []
        for i in range(8):
            inv.append(1.0 / d[i, i])
            for j in range(i + 1, 8):
                coef = d[i, j] * inv[i]
                r[j] = r[j] - coef * r[i]
                for k in range(j, 8):
                    d[j, k] = d[j, k] - coef * d[i, k]
        scaled = [r[i] * inv[i] for i in range(8)]
        for t in range(base + 8, rows):
            row = aug[t]
            acc = [None, None]
            for i in range(8):
                term = jnp.broadcast_to(scaled[i][:, t : t + 1], (8, 128)) * r[i]
                acc[i % 2] = term if acc[i % 2] is None else acc[i % 2] + term
            aug[t] = row - (acc[0] + acc[1])
        for i in range(8):
            aug[base + i] = r[i] / jnp.sqrt(d[i, i])
        yield


def orthonormalize(p_src, pt_out, aug, s_ref):
    eye = (lax.broadcasted_iota(jnp.int32, (RANK, 128), 0) + RANK == lax.broadcasted_iota(jnp.int32, (RANK, 128), 1)).astype(F32)
    for rep in range(2):
        for m in range(6, 8):
            aug[:, m, :] = jnp.where(lax.broadcasted_iota(jnp.int32, (RANK, 128), 0) == lax.broadcasted_iota(jnp.int32, (RANK, 128), 1), 1.0, eye)
        for m in range(6):
            pt = p_src(m) if rep == 0 else pt_out[m]
            gram = full_dot(pt, pt, NT)
            aug[:, m, :] = jnp.concatenate([gram, jnp.zeros((RANK, RANK), F32)], axis=1) + eye
        yield
        yield from eliminate(aug)
        for m in range(6):
            s_new = aug[:, m, :][:, RANK:]
            pt = p_src(m) if rep == 0 else pt_out[m]
            pt_out[m] = full_dot(s_new, pt, NN)
            s_ref[m] = s_new if rep == 0 else full_dot(s_new, s_ref[m], NN)
        yield


def reduce_kernel(num_dev, gp, gu, ep, eu, qp, qu, wp, wu, vp, vu,
                  m_out, w_out, v_out, qt_out, pt_out,
                  gbuf, xp, rap, rbp, rcp, rp, xq, raq, rbq, rcq, rq, aug, s_ref,
                  esem, gsem, qsem, wsem, ssem, rsem):
    place = Place()
    barrier = pltpu.get_barrier_semaphore()
    peers = [place.partner] + place.mates + place.zmates
    for dev in peers:
        pl.semaphore_signal(barrier, inc=1, device_id=(dev,), device_id_type=MESH)

    def load(ci):
        l, c, slot = ci // PER_LAYER, ci % PER_LAYER, ci % SLOTS

        @pl.when(c == 0)
        def _():
            pltpu.make_async_copy(ep.at[l], m_out.at[ci], esem.at[slot]).start()
            pltpu.make_async_copy(gp.at[l], gbuf.at[slot], gsem.at[slot]).start()

        @pl.when(c > 0)
        def _():
            cols = pl.ds(pl.multiple_of((c - 1) * BLK, BLK), BLK)
            pltpu.make_async_copy(eu.at[l, :, cols], m_out.at[ci], esem.at[slot]).start()
            pltpu.make_async_copy(gu.at[l, :, cols], gbuf.at[slot], gsem.at[slot]).start()

    qcopies = []
    for l in range(LAYERS):
        for c in range(PER_LAYER):
            ci = l * PER_LAYER + c
            src = qp.at[l] if c == 0 else qu.at[l, :, pl.ds((c - 1) * BLK, BLK)]
            qcopies.append(pltpu.make_async_copy(src, rq.at[l, :, pl.ds(c * BLK, BLK)], qsem.at[ci]))
    for cp in qcopies[:PER_LAYER]:
        cp.start()
    for ci in range(SLOTS):
        load(ci)
    for cp in qcopies[PER_LAYER:]:
        cp.start()

    punit = [Unit(place, (xp.at[l], rap.at[l], rbp.at[l], rcp.at[l]), rp.at[l], (ssem.at[l], rsem.at[l]), num_dev) for l in range(LAYERS)]
    qunit = [Unit(place, (xq.at[l], raq.at[l], rbq.at[l], rcq.at[l]), rq.at[l], (ssem.at[3 + l], rsem.at[3 + l]), num_dev) for l in range(LAYERS)]

    def p_layer(l):
        xp[l] = jnp.zeros((RANK, P_COLS), F32)
        for c in range(PER_LAYER):
            qcopies[l * PER_LAYER + c].wait()

        @pl.loop(0, PER_LAYER)
        def _(c):
            ci = l * PER_LAYER + c
            slot = ci % SLOTS
            pltpu.make_async_copy(ep.at[0], m_out.at[ci], esem.at[slot]).wait()
            pltpu.make_async_copy(gp.at[0], gbuf.at[slot], gsem.at[slot]).wait()
            mat = m_out[ci] + gbuf[slot].astype(F32)
            m_out[ci] = mat
            cols = pl.ds(pl.multiple_of(jnp.minimum(c, 1) * BLK, BLK), BLK)
            fac = rq[l, :, pl.ds(pl.multiple_of(c * BLK, BLK), BLK)]
            xp[l, :, cols] += stacked_dot(fac, mat, NT)

            @pl.when(ci + SLOTS < CHUNKS)
            def _():
                load(ci + SLOTS)

    def q_layer(l):
        @pl.loop(0, PER_LAYER)
        def _(c):
            ci = l * PER_LAYER + c
            cols = pl.ds(pl.multiple_of(jnp.minimum(c, 1) * BLK, BLK), BLK)
            out = pl.ds(pl.multiple_of(c * BLK, BLK), BLK)
            xq[l, :, out] = stacked_dot(rp[l, :, cols], m_out[ci], NN)

    wcopies = []
    for l in range(LAYERS):
        for c in range(PER_LAYER):
            ci = l * PER_LAYER + c
            for t, (sp, su, dst) in enumerate(((wp, wu, w_out), (vp, vu, v_out))):
                src = sp.at[l] if c == 0 else su.at[l, :, pl.ds((c - 1) * BLK, BLK)]
                wcopies.append(pltpu.make_async_copy(src, dst.at[ci], wsem.at[2 * ci + t]))

    p_layer(0)
    pl.semaphore_wait(barrier, len(peers))
    punit[0].stage(0)
    p_layer(1)
    punit[0].stage(1)
    punit[1].stage(0)
    p_layer(2)
    punit[0].stage(2)
    punit[1].stage(1)
    punit[2].stage(0)
    for cp in wcopies:
        cp.start()
    for tick in range(4):
        punit[0].stage(tick + 3)
        punit[1].stage(tick + 2)
        punit[2].stage(tick + 1)
    q_layer(0)
    qunit[0].stage(0)
    punit[1].stage(6)
    punit[2].stage(5)
    q_layer(1)
    qunit[1].stage(0)
    qunit[0].stage(1)
    punit[2].stage(6)
    q_layer(2)
    qunit[2].stage(0)
    qunit[1].stage(1)
    qunit[0].stage(2)

    def p_src(m):
        return rp[m // 2, :, (m % 2) * BLK : (m % 2) * BLK + BLK]

    work = orthonormalize(p_src, pt_out, aug, s_ref)
    steps = []
    for tick in range(6):
        for l in range(LAYERS):
            num = tick + 3 - l
            if num <= 6:
                steps.append((l, num))
    for l, num in steps:
        next(work, None)
        qunit[l].stage(num)
    for _ in work:
        pass
    for l in range(LAYERS):
        for c in range(PER_LAYER):
            qt_out[l * PER_LAYER + c] = full_dot(s_ref[2 * l + min(c, 1)], rq[l, :, c * BLK : (c + 1) * BLK], NN)
    for unit in punit + qunit:
        unit.finish()
    for cp in wcopies:
        cp.wait()


def apply_kernel(m_in, w_in, v_in, qt_in, pt_in, wp, wu, vp, vu, qp, qu, ep, eu, lhs, buf, sem, qsem):
    qcopies = []
    for l in range(LAYERS):
        for c in range(PER_LAYER):
            ci = l * PER_LAYER + c
            dst = qp.at[l] if c == 0 else qu.at[l, :, pl.ds((c - 1) * BLK, BLK)]
            qcopies.append(pltpu.make_async_copy(qt_in.at[ci], dst, qsem.at[ci]))
    for cp in qcopies:
        cp.start()

    @pl.loop(0, 2 * LAYERS)
    def _(m):
        p1, p2, p3 = [t.astype(F32) for t in split3(pt_in[m])]
        for t, (a, b) in enumerate(((p1, p1), (p2, p1), (p2, p3))):
            lhs[m, :, 128 * t : 128 * t + 128] = jnp.transpose(jnp.concatenate([a, b], axis=0)).astype(BF16)

    outs = ((ep, eu), (vp, vu), (wp, wu))

    @pl.loop(0, 2 * CHUNKS)
    def _(step):
        ci, slot = step // 2, step % SLOTS
        l, c = ci // PER_LAYER, ci % PER_LAYER
        rows = pl.ds(pl.multiple_of((step % 2) * HALF, HALF), HALF)

        @pl.when(step >= SLOTS)
        def _():
            for t in range(3):
                pltpu.make_async_copy(buf.at[slot, t], ep.at[0, pl.ds(0, HALF)], sem.at[slot, t]).wait()

        q1, q2, q3 = split3(qt_in[ci])
        rhs = jnp.concatenate([q1, q2, q1, q3, q2, q1], axis=0)
        hat = mxu(lhs[2 * l + jnp.minimum(c, 1), rows], rhs, NN)
        buf[slot, 0] = m_in[ci, rows] - hat
        mom = MOMENTUM * v_in[ci, rows] + hat
        buf[slot, 1] = mom
        buf[slot, 2] = w_in[ci, rows] - LEARN_RATE * mom

        @pl.when(c == 0)
        def _():
            for t in range(3):
                pltpu.make_async_copy(buf.at[slot, t], outs[t][0].at[l, rows], sem.at[slot, t]).start()

        @pl.when(c > 0)
        def _():
            cols = pl.ds(pl.multiple_of((c - 1) * BLK, BLK), BLK)
            for t in range(3):
                pltpu.make_async_copy(buf.at[slot, t], outs[t][1].at[l, rows, cols], sem.at[slot, t]).start()

    for slot in range(SLOTS):
        for t in range(3):
            pltpu.make_async_copy(buf.at[slot, t], ep.at[0, pl.ds(0, HALF)], sem.at[slot, t]).wait()
    for cp in qcopies:
        cp.wait()


def solution(mesh):
    num_dev = mesh.shape['dp']
    dev_spec, rep_spec = P('dp'), P()
    sds = jax.ShapeDtypeStruct
    hbm, vmem = pl.BlockSpec(memory_space=pltpu.HBM), pl.BlockSpec(memory_space=pltpu.VMEM)
    big = pltpu.VMEM((CHUNKS, BLK, BLK), F32)

    def bufs(cols):
        return [pltpu.VMEM((LAYERS, RANK, cols), F32), pltpu.VMEM((LAYERS, 32, cols), F32),
                pltpu.VMEM((LAYERS, 3, 8, cols), F32), pltpu.VMEM((LAYERS, 3, 8, cols // 4), F32),
                pltpu.VMEM((LAYERS, RANK, cols), F32)]

    def local_step(grad_p, grad_u, err_p, err_u, q_p, q_u, w_p, w_u, mom_p, mom_u):
        m_all, w_all, v_all, qt, pt = pl.pallas_call(
            lambda *refs: reduce_kernel(num_dev, *refs),
            out_shape=[big, big, big, pltpu.VMEM((CHUNKS, RANK, BLK), F32), pltpu.VMEM((2 * LAYERS, RANK, BLK), F32)],
            in_specs=[hbm] * 10,
            out_specs=[vmem] * 5,
            scratch_shapes=[pltpu.VMEM((SLOTS, BLK, BLK), BF16)]
            + bufs(P_COLS) + bufs(Q_COLS)
            + [pltpu.VMEM((RANK, 8, 128), F32), pltpu.VMEM((2 * LAYERS, RANK, RANK), F32),
               pltpu.SemaphoreType.DMA((SLOTS,)), pltpu.SemaphoreType.DMA((SLOTS,)),
               pltpu.SemaphoreType.DMA((CHUNKS,)), pltpu.SemaphoreType.DMA((2 * CHUNKS,)),
               pltpu.SemaphoreType.DMA((6, 14)), pltpu.SemaphoreType.DMA((6, 14))],
            compiler_params=pltpu.CompilerParams(collective_id=0, has_side_effects=True, vmem_limit_bytes=VMEM_LIMIT),
            name='reduce_factors',
        )(grad_p[0], grad_u[0], err_p[0], err_u[0], jnp.swapaxes(q_p, 1, 2), jnp.swapaxes(q_u, 1, 2), w_p, w_u, mom_p, mom_u)
        small, wide = sds((LAYERS, BLK, BLK), F32), sds((LAYERS, BLK, 4 * BLK), F32)
        w_pn, w_un, v_pn, v_un, q_pn, q_un, e_pn, e_un = pl.pallas_call(
            apply_kernel,
            out_shape=[small, wide, small, wide, sds((LAYERS, RANK, BLK), F32), sds((LAYERS, RANK, 4 * BLK), F32), small, wide],
            in_specs=[vmem] * 5,
            out_specs=[hbm] * 8,
            scratch_shapes=[pltpu.VMEM((2 * LAYERS, BLK, 384), BF16), pltpu.VMEM((SLOTS, 3, HALF, BLK), F32),
                            pltpu.SemaphoreType.DMA((SLOTS, 3)), pltpu.SemaphoreType.DMA((CHUNKS,))],
            compiler_params=pltpu.CompilerParams(vmem_limit_bytes=VMEM_LIMIT),
            name='apply_factors',
        )(*[pltpu.with_memory_space_constraint(t, pltpu.VMEM) for t in (m_all, w_all, v_all, qt, pt)])
        return (w_pn, w_un, v_pn, v_un, jnp.swapaxes(q_pn, 1, 2), jnp.swapaxes(q_un, 1, 2), e_pn[None], e_un[None])

    in_specs = (dev_spec,) * 4 + (rep_spec,) * 6
    out_specs = (rep_spec,) * 6 + (dev_spec,) * 2
    return jax.shard_map(local_step, mesh=mesh, in_specs=in_specs, out_specs=out_specs, check_vma=False)
```
